256 devices in a mesh: section: 8 (over z), ctx: 32 (over x, y, core).
Axes of the slice: x: 4, y: 4, z: 8, core: 2. Of those that a mesh axis runs over, the one named last changes fastest.
Arguments:
- queries: bfloat16 [8, 8192, 3072], P('section', 'ctx'), may hold values from -160 to 160
- keys: bfloat16 [8, 8192, 512], P('section', 'ctx'), may hold values from -48 to 48
- values: bfloat16 [8, 8192, 512], P('section', 'ctx'), may hold values from -15 to 15
- cotangent: bfloat16 [8, 8192, 3072], P('section', 'ctx'), may hold values from -6 to 6
- router_logits: bfloat16 [8, 8192], P('section', 'ctx'), may hold values from -8 to 8
- positions: int32 [8, 8192], P('section', 'ctx'), may hold values from -1 to 32767, as said below
- counts: int32 [8, 32], P('section', 'ctx'), may hold values from 0 to 2, as said below
Outputs:
- handed: bfloat16 [8, 8192, 3072], P('section', 'ctx')
- value_grad: bfloat16 [8, 8192, 512], P('section', 'ctx')
- gate_grad: bfloat16 [8, 8192], P('section', 'ctx')
The draws below stay inside these ranges and needn't reach their ends.
Inputs may be any that keep to these rules, and one draw needn't show every extreme that they name: For every micro-batch and every shard c, the counts of shards 0 to c sum to c + 1 or c + 2; shard 0 holds 2 blocks; all counts of a micro-batch sum to 32. In shard c's slots, the first counts * 128 hold distinct positions in increasing order, all within c * 1024 to (c + 1) * 1024 - 1; the other slots hold -1.
All inputs are finite; a program needn't handle non-finite values.
Results may differ from the reference program's by a relative error of at most 0.0066.
Values may be sent and summed in bfloat16 or wider, within the bound.
A program may use at most 128 MiB of HBM per device.

```python
import math
import jax
import jax.numpy as jnp
from jax import lax

QUERY_HEADS = 24
KEY_VALUE_HEADS = 4
HEAD_SIZE = 128
BLOCK_ROWS = 128
MAXB = 2
TOK_DEV = 1024
ROUTED_SLOTS = 8192
MICRO_BATCHES = 8
N_CTX = 32


def block_counts(key):
    carry_key = jax.random.fold_in(key, 11)
    carry_bits = jax.random.randint(carry_key, (MICRO_BATCHES, N_CTX), 0, 2).astype(jnp.int32)
    column = jnp.arange(N_CTX)[None, :]
    carry_bits = jnp.where(column == 0, 1, jnp.where(column == N_CTX - 1, 0, carry_bits)).astype(jnp.int32)
    carry_before = jnp.concatenate([jnp.zeros((MICRO_BATCHES, 1), jnp.int32), carry_bits[:, :-1]], axis=1)
    return (1 + carry_bits - carry_before).astype(jnp.int32)


def draw_counts(key, part):
    return block_counts(key)


def draw_positions(key, part):
    held_blocks = block_counts(key)
    slot_total = MAXB * BLOCK_ROWS
    noise_key = jax.random.fold_in(key, 23)
    noise_draw = jax.random.randint(noise_key, (MICRO_BATCHES, N_CTX, TOK_DEV), 0, 1 << 16)
    sort_scores = noise_draw * TOK_DEV + jnp.arange(TOK_DEV, dtype=jnp.int32)[None, None, :]
    shuffled = jnp.argsort(sort_scores, axis=-1)[..., :slot_total].astype(jnp.int32)
    slot_index = jnp.arange(slot_total, dtype=jnp.int32)[None, None, :]
    live_slot = slot_index < held_blocks[..., None] * BLOCK_ROWS
    sort_keys = jnp.where(live_slot, shuffled, shuffled + TOK_DEV)
    ranked = jnp.sort(sort_keys, axis=-1)
    shard_start = jnp.arange(N_CTX, dtype=jnp.int32)[None, :, None] * TOK_DEV
    placed = jnp.where(live_slot, ranked + shard_start, -1)
    return placed.reshape(MICRO_BATCHES, N_CTX * slot_total).astype(jnp.int32)


def head_draws(key):
    query_group_width = QUERY_HEADS // KEY_VALUE_HEADS
    total_row_count = N_CTX * MAXB * BLOCK_ROWS
    base_key = jax.random.fold_in(key, 37)
    random_key_first = jax.random.fold_in(base_key, 0)
    random_key_fifth = jax.random.fold_in(base_key, 4)
    key_row_block = 2.0 * jnp.clip(jax.random.normal(random_key_first, (MICRO_BATCHES, total_row_count, KEY_VALUE_HEADS, HEAD_SIZE)), -6.0, 6.0)
    query_row_block = jnp.clip(jax.random.normal(random_key_fifth, (MICRO_BATCHES, total_row_count, KEY_VALUE_HEADS, query_group_width, HEAD_SIZE)), -6.0, 6.0)
    return (query_row_block.reshape(MICRO_BATCHES, total_row_count, QUERY_HEADS * HEAD_SIZE), key_row_block.reshape(MICRO_BATCHES, total_row_count, KEY_VALUE_HEADS * HEAD_SIZE))


def draw_queries(key, part):
    return head_draws(key)[0].astype(jnp.bfloat16)


def draw_keys(key, part):
    return head_draws(key)[1].astype(jnp.bfloat16)


def levels(own_key, shape, cuts, low, top_value):
    loudness = 1.0
    for axis_at, blocks in cuts:
        heights = jax.random.uniform(jax.random.fold_in(jax.random.fold_in(own_key, 6), axis_at), (blocks,), jnp.float32, low / len(cuts), top_value / len(cuts))
        loudness = loudness * jnp.repeat(jnp.exp(heights), shape[axis_at] // blocks).reshape((-1,) + (1,) * (len(shape) - 1 - axis_at))
    return loudness


def gaussian(stream_key, shape, width, bound, shards=(), kind=jnp.bfloat16):
    drawn = width * jax.random.normal(stream_key, shape, jnp.float32)
    if shards:
        drawn = drawn * levels(stream_key, shape, shards, -0.22, 0.18)
    return jnp.clip(drawn, -bound, bound).astype(kind)


def setup_inputs(seed: int = 0) -> dict:
    arg_keys = jax.random.split(jax.random.key(seed), 8)
    queries = draw_queries(jax.random.fold_in(arg_keys[7], 71), 0)
    keys = draw_keys(jax.random.fold_in(arg_keys[7], 71), 0)
    values = gaussian(arg_keys[2], (MICRO_BATCHES, ROUTED_SLOTS, KEY_VALUE_HEADS * HEAD_SIZE), 3.0, 15.0, ((0, 8), (1, 32)))
    cotangent = gaussian(arg_keys[3], (MICRO_BATCHES, ROUTED_SLOTS, QUERY_HEADS * HEAD_SIZE), 1.0, 6.0, ((0, 8), (1, 32)))
    router_logits = gaussian(arg_keys[4], (MICRO_BATCHES, ROUTED_SLOTS), 2.0, 8.0, ((0, 8), (1, 32)))
    positions = draw_positions(jax.random.fold_in(arg_keys[7], 71), 0)
    counts = draw_counts(jax.random.fold_in(arg_keys[7], 71), 0)
    return dict(queries=queries, keys=keys, values=values, cotangent=cotangent, router_logits=router_logits, positions=positions, counts=counts)


def block_order(blocks_held):
    inclusive = jnp.cumsum(blocks_held).astype(jnp.int32)
    target = jnp.arange(N_CTX, dtype=jnp.int32)
    owner_shard = lax.optimization_barrier(jnp.sum((inclusive[None, :] <= target[:, None]).astype(jnp.int32), axis=1)).astype(jnp.int32)
    first_block = (inclusive - blocks_held).astype(jnp.int32)
    local_block = (target - first_block[owner_shard]).astype(jnp.int32)
    return (owner_shard * MAXB + local_block).astype(jnp.int32)

def one_section(bundle):
    queries, keys, values, cotangent, logits, places, blocks_held = bundle
    dense_order = block_order(blocks_held)
    query_group_width = QUERY_HEADS // KEY_VALUE_HEADS

    def sorted_positions(source):
        shaped = source.reshape((N_CTX * MAXB, BLOCK_ROWS) + source.shape[1:])
        return shaped[dense_order].reshape((N_CTX * BLOCK_ROWS,) + source.shape[1:])
    key_head_rows = sorted_positions(keys).astype(jnp.float32).reshape(N_CTX * BLOCK_ROWS, KEY_VALUE_HEADS, HEAD_SIZE)
    value_head_rows = sorted_positions(values).astype(jnp.float32).reshape(N_CTX * BLOCK_ROWS, KEY_VALUE_HEADS, HEAD_SIZE)
    key_places = sorted_positions(places)
    query_block_list = sorted_positions(queries).reshape(N_CTX, BLOCK_ROWS, KEY_VALUE_HEADS, query_group_width, HEAD_SIZE)
    grad_blocks = sorted_positions(cotangent).reshape(N_CTX, BLOCK_ROWS, QUERY_HEADS * HEAD_SIZE)
    logit_blocks = sorted_positions(logits).reshape(N_CTX, BLOCK_ROWS)
    place_blocks = key_places.reshape(N_CTX, BLOCK_ROWS)

    def per_block(grad_total, block_parts):
        query_part, grad_part, logit_part, place_part = block_parts
        scores = jnp.einsum('qhgd,khd->hgqk', query_part.astype(jnp.float32), key_head_rows) / math.sqrt(HEAD_SIZE)
        allowed = key_places[None, :] <= place_part[:, None]
        row_top = lax.optimization_barrier(jnp.max(jnp.where(allowed, scores, -jnp.inf), axis=-1))
        weights = jnp.where(allowed, jnp.exp(scores - row_top[..., None]), 0.0)
        weight_sum = lax.optimization_barrier(jnp.sum(weights, axis=-1))
        rounded = lax.optimization_barrier(weights.astype(jnp.bfloat16)).astype(jnp.float32)
        attended = jnp.einsum('hgqk,khd->qhgd', rounded, value_head_rows)
        attended = attended / jnp.transpose(weight_sum, (2, 0, 1))[..., None]
        attended = attended.reshape(BLOCK_ROWS, QUERY_HEADS * HEAD_SIZE)
        gate_values = jax.nn.sigmoid(logit_part.astype(jnp.float32))
        branch = (gate_values[:, None] * attended).astype(jnp.bfloat16)
        log_total = row_top + jnp.log(weight_sum)
        gradient_broad = grad_part.astype(jnp.float32)
        output_gradient = lax.optimization_barrier((gate_values[:, None] * gradient_broad).astype(jnp.bfloat16)).astype(jnp.float32)
        output_gradient = output_gradient.reshape(BLOCK_ROWS, KEY_VALUE_HEADS, query_group_width, HEAD_SIZE)
        probabilities = jnp.where(allowed, jnp.exp(scores - log_total[..., None]), 0.0)
        probabilities = lax.optimization_barrier(probabilities.astype(jnp.bfloat16)).astype(jnp.float32)
        grad_total = grad_total + jnp.einsum('hgqk,qhgd->khd', probabilities, output_gradient)
        gate_term = (gate_values * (1.0 - gate_values) * lax.optimization_barrier(jnp.sum(gradient_broad * attended, axis=1))).astype(jnp.bfloat16)
        return (grad_total, (branch, gate_term))
    initial_gradient = jnp.zeros((N_CTX * BLOCK_ROWS, KEY_VALUE_HEADS, HEAD_SIZE), jnp.float32)
    value_grand_sum, outputs = lax.scan(per_block, initial_gradient, (query_block_list, grad_blocks, logit_blocks, place_blocks))
    branches, gate_terms = outputs

    def to_owner(dense_rows):
        tail = dense_rows.shape[2:]
        empty_slots = jnp.zeros((N_CTX * MAXB, BLOCK_ROWS) + tail, dense_rows.dtype)
        return empty_slots.at[dense_order].set(dense_rows).reshape((N_CTX * MAXB * BLOCK_ROWS,) + tail)
    value_finished = value_grand_sum.astype(jnp.bfloat16).reshape(N_CTX, BLOCK_ROWS, KEY_VALUE_HEADS * HEAD_SIZE)
    return (to_owner(branches), to_owner(value_finished), to_owner(gate_terms))

def reference(queries, keys, values, cotangent, router_logits, positions, counts):
    branch_all, value_grad, gate_grad = lax.map(one_section, (queries, keys, values, cotangent, router_logits, positions, counts))
    handed = jnp.roll(branch_all, 1, axis=0)
    return (handed, value_grad, gate_grad)
```

```python
import math

import jax
import jax.numpy as jnp
from jax import lax
from jax.experimental import pallas as pl
from jax.experimental.pallas import tpu as pltpu
from jax.sharding import PartitionSpec as P

GROUPS = 4
WIDE = 6
D = 128
B = 128
COLS = WIDE * D
SECTIONS = 8
CTX = 32
TILE = 512
LOW = -1e30
SCALE = math.log2(math.e) / math.sqrt(D)
BF = jnp.bfloat16
F32 = jnp.float32
NCOPY = 260


def kernel(
    counts, q_in, k_in, v_in, ct_in, lg_in,
    handed, vgrad, ggrad,
    cb, qs, qr, cs, cr, ks, kr, vs, vr, ls, lr, gs, gr, fl, flr,
    kb, vb, sbuf, wbuf, qt, ot, dos, att_acc,
    pda, pdb, rba, rbb, ra, rb, ua, ub, ra2, rb2, dvf, dvr,
    br, hz, hr, csem, send_sems, recv_sems,
):
    sec = lax.axis_index("section")
    c = lax.axis_index("ctx")
    core = lax.rem(c, 2)
    y = lax.rem(lax.div(c, 2), 4)
    x = lax.div(c, 8)

    def dev(xx, yy, kk):
        return (sec, (lax.rem(xx + 8, 4) * 4 + lax.rem(yy + 8, 4)) * 2 + kk)

    nxt = (sec, lax.rem(c + 1, CTX))
    prv = (sec, lax.rem(c + CTX - 1, CTX))
    zup = (lax.rem(sec + 1, SECTIONS), c)
    zdn = (lax.rem(sec + SECTIONS - 1, SECTIONS), c)
    sib = (sec, c + 1 - 2 * core)
    MESH = pl.DeviceIdType.MESH

    made = []
    slots = {}

    def copy(name, src, dst, to):
        n = slots.setdefault(name, len(slots))
        made.append(
            pltpu.make_async_remote_copy(
                src_ref=src, dst_ref=dst, send_sem=send_sems.at[n], recv_sem=recv_sems.at[n],
                device_id=to, device_id_type=MESH,
            )
        )
        made[-1].start()
        return made[-1]

    def arrived(name, dst):
        n = slots[name]
        pltpu.make_async_remote_copy(
            src_ref=dst, dst_ref=dst, send_sem=send_sems.at[n], recv_sem=recv_sems.at[n],
            device_id=sib, device_id_type=MESH,
        ).wait_recv()

    bar = pltpu.get_barrier_semaphore()

    @pl.loop(1, CTX)
    def _(d):
        pl.semaphore_signal(bar, inc=1, device_id=(sec, lax.rem(c + d, CTX)), device_id_type=MESH)

    pl.semaphore_signal(bar, inc=1, device_id=zup, device_id_type=MESH)
    pl.semaphore_signal(bar, inc=1, device_id=zdn, device_id_type=MESH)

    held = counts[0, 0]
    two = held == 2
    cb[pl.ds(c, 1)] = jnp.full((1, 8, 128), held, jnp.int32)

    def pick(flag, a, b):
        return lax.select(jnp.broadcast_to(flag, a.shape), a, b)

    for g in range(GROUPS):
        kc = slice(g * D, (g + 1) * D)
        qc = slice(g * COLS, (g + 1) * COLS)
        ks[g] = pick(two, k_in[B:, kc], k_in[:B, kc])
        vs[g] = pick(two, v_in[B:, kc], v_in[:B, kc])
        qs[g] = pick(two, q_in[B:, qc], q_in[:B, qc])
        cs[g] = pick(two, ct_in[B:, qc], ct_in[:B, qc])
    lg = lg_in[...].astype(F32)
    ls[...] = jnp.broadcast_to(pick(two, lg[:, B:], lg[:, :B]), (8, 128))

    pl.semaphore_wait(bar, CTX + 1)

    @pl.loop(1, CTX)
    def _(d):
        pltpu.make_async_remote_copy(
            src_ref=cb.at[c], dst_ref=cb.at[c], send_sem=csem.at[0], recv_sem=csem.at[1],
            device_id=(sec, lax.rem(c + d, CTX)), device_id_type=MESH,
        ).start()

    copy("k", ks, kr, nxt)
    copy("v", vs, vr, nxt)
    copy("l", ls, lr, nxt)
    for g in range(GROUPS):
        copy(("q", g), qs.at[g], qr.at[g], nxt)
    for g in range(GROUPS):
        copy(("c", g), cs.at[g], cr.at[g], nxt)

    every = pltpu.make_async_remote_copy(
        src_ref=cb.at[pl.ds(0, CTX - 1)], dst_ref=cb.at[pl.ds(0, CTX - 1)],
        send_sem=csem.at[0], recv_sem=csem.at[1], device_id=sib, device_id_type=MESH,
    )
    every.wait_recv()
    order = lax.broadcasted_iota(jnp.int32, (CTX, 8, 128), 0)
    ahead = jnp.sum(jnp.where(order < c, cb[...] - 1, 0), axis=0).astype(F32)
    before = jnp.max(ahead)
    late = before > 0.5
    held_f = held.astype(F32)
    fl[0] = ahead
    fl[1] = jnp.full((8, 128), held_f, F32)

    arrived("k", kr)
    arrived("v", vr)
    for g in range(GROUPS):
        kc = slice(g * D, (g + 1) * D)
        kb[g, core, y, x] = pick(late, kr[g], k_in[:B, kc])
        vb[g, core, x, y] = pick(late, vr[g], v_in[:B, kc])
    copy("f", fl, flr, zup)

    def at(v):
        return lax.rem(v + 8, 4)

    for g in range(GROUPS):
        for d in (1, 3, 2):
            copy(("k1", g, d), kb.at[g, core, y, x], kb.at[g, core, y, x], dev(x + d, y, core))
            copy(("v1", g, d), vb.at[g, core, x, y], vb.at[g, core, x, y], dev(x, y + d, core))

    def gather_second(g):
        for d in (1, 3, 2):
            arrived(("k1", g, d), kb.at[g, core, y, at(x - d)])
            arrived(("v1", g, d), vb.at[g, core, x, at(y - d)])
        for d in (1, 3):
            copy(("k2", g, d), kb.at[g, core, y], kb.at[g, core, y], dev(x, y + d, core))
            copy(("v2", g, d), vb.at[g, core, x], vb.at[g, core, x], dev(x + d, y, core))
        copy(("kd", g, 0), kb.at[g, core, y], kb.at[g, core, y], sib)
        copy(("vd", g, 0), vb.at[g, core, x], vb.at[g, core, x], sib)

    def gather_third(g):
        for d in (1, 3):
            part = pl.ds(0, 2) if d == 1 else pl.ds(2, 2)
            yy, xx = at(y - d), at(x - d)
            arrived(("k2", g, d), kb.at[g, core, yy])
            copy(("k3", g, d), kb.at[g, core, yy, part], kb.at[g, core, yy, part], dev(x, y + d, core))
            arrived(("v2", g, d), vb.at[g, core, xx])
            copy(("v3", g, d), vb.at[g, core, xx, part], vb.at[g, core, xx, part], dev(x + d, y, core))
            copy(("kd", g, d), kb.at[g, core, yy], kb.at[g, core, yy], sib)
            copy(("vd", g, d), vb.at[g, core, xx], vb.at[g, core, xx], sib)

    def gather_fourth(g):
        yy, xx = at(y + 2), at(x + 2)
        for d in (1, 3):
            part = pl.ds(0, 2) if d == 1 else pl.ds(2, 2)
            arrived(("k3", g, d), kb.at[g, core, yy, part])
            arrived(("v3", g, d), vb.at[g, core, xx, part])
        copy(("kd", g, 2), kb.at[g, core, yy], kb.at[g, core, yy], sib)
        copy(("vd", g, 2), vb.at[g, core, xx], vb.at[g, core, xx], sib)

    def gather_last(g):
        for d in (0, 1, 3, 2):
            arrived(("kd", g, d), kb.at[g, 1 - core, at(y - d)])
            arrived(("vd", g, d), vb.at[g, 1 - core, at(x - d)])

    tiles = lax.div(c, 4) + 1
    lane = lax.broadcasted_iota(jnp.int32, (TILE, 2 * D), 1)
    gap = lax.broadcasted_iota(jnp.int32, (TILE, 2 * D), 0) - lax.rem(lane, D)

    def forward(g):
        arrived(("q", g), qr.at[g])
        qc = slice(g * COLS, (g + 1) * COLS)
        for h in range(WIDE):
            hc = slice(h * D, (h + 1) * D)
            full = pick(late, qr[g, :, hc], q_in[:B, g * COLS + h * D : g * COLS + (h + 1) * D])
            full = (full.astype(F32) * SCALE).T
            high = full.astype(BF)
            qt[:D, hc] = high
            qt[D:, hc] = (full - high.astype(F32)).astype(BF)

        def scores(j, tops):
            xx, y0 = lax.div(j, 2), lax.rem(j, 2) * 2
            one = jnp.concatenate(
                [kb[g, 0, y0, xx], kb[g, 1, y0, xx], kb[g, 0, y0 + 1, xx], kb[g, 1, y0 + 1, xx]], axis=0
            )
            both = jnp.concatenate([one, one], axis=1)
            bound = c * B - j * TILE
            out = []
            for p in range(3):
                pc = slice(p * 2 * D, (p + 1) * 2 * D)
                s = jnp.dot(both, qt[:, pc], preferred_element_type=F32)
                s = jnp.where(gap <= bound, s, LOW)
                sbuf[pl.ds(pl.multiple_of(j * TILE, TILE), TILE), pc] = s
                out.append(jnp.maximum(tops[p], jnp.max(s.reshape(TILE // 8, 8, 2 * D), axis=0)))
            return tuple(out)

        tops = lax.fori_loop(
            0, tiles, scores, tuple(jnp.full((8, 2 * D), LOW, F32) for _ in range(3))
        )
        tops = [jnp.max(t, axis=0, keepdims=True) for t in tops]
        ot[...] = jnp.zeros_like(ot)

        def weigh(j, _):
            xx, y0 = lax.div(j, 2), lax.rem(j, 2) * 2
            one = jnp.concatenate(
                [vb[g, 0, xx, y0], vb[g, 1, xx, y0], vb[g, 0, xx, y0 + 1], vb[g, 1, xx, y0 + 1]], axis=0
            )
            left = jnp.concatenate([one.T, jnp.ones((16, TILE), BF)], axis=0)
            rows = pl.ds(pl.multiple_of(j * TILE, TILE), TILE)
            for p in range(3):
                pc = slice(p * 2 * D, (p + 1) * 2 * D)
                w = jnp.exp2(sbuf[rows, pc] - tops[p]).astype(BF)
                wbuf[rows, pc] = w
                ot[:, pc] += jnp.dot(left, w, preferred_element_type=F32)
            return 0

        lax.fori_loop(0, tiles, weigh, 0)
        if g == 0:
            arrived("l", lr)
            gate_row = 1.0 / (1.0 + jnp.exp(-pick(late, lr[...], jnp.broadcast_to(lg[:, :B], (8, 128)))))
            gr[...] = gate_row
            att_acc[0] = jnp.broadcast_to(gate_row[:1], (B, D)).T
            att_acc[1] = jnp.zeros((B, D), F32)
        arrived(("c", g), cr.at[g])
        gate = att_acc[0]
        acc = att_acc[1]
        for h in range(WIDE):
            hc = slice(h * D, (h + 1) * D)
            inv = 1.0 / ot[D : D + 1, hc]
            attended = (ot[:D, hc] * inv).T
            br[g, :, hc] = (gate * attended).astype(BF)
            ct = pick(late, cr[g, :, hc], ct_in[:B, g * COLS + h * D : g * COLS + (h + 1) * D]).astype(F32)
            acc = acc + ct * attended
            dos[hc, :] = (gate * ct * jnp.broadcast_to(inv, (B, D)).T).astype(BF)
        att_acc[1] = acc
        copy(("h", g), br.at[g], hz.at[g], zup)

    def backward(g):
        def terms(j, _):
            xx, y0 = lax.div(j, 2), lax.rem(j, 2) * 2
            rows = pl.ds(pl.multiple_of(j * TILE, TILE), TILE)
            t = jnp.dot(wbuf[rows, :], dos[...], preferred_element_type=F32).astype(BF)
            for n in range(4):
                pda[g, n % 2, xx, y0 + n // 2] = t[n * B : n * B + 64]
                pdb[g, n % 2, y0 + n // 2, xx] = t[n * B + 64 : (n + 1) * B]
            return 0

        lax.fori_loop(0, tiles, terms, 0)

        def blank(j, _):
            xx, y0 = lax.div(j, 2), lax.rem(j, 2) * 2
            for n in range(4):
                pda[g, n % 2, xx, y0 + n // 2] = jnp.zeros((64, D), BF)
                pdb[g, n % 2, y0 + n // 2, xx] = jnp.zeros((64, D), BF)
            return 0

        lax.fori_loop(tiles, CTX // 4, blank, 0)
        copy(("a0", g), pda.at[g, 1 - core], rba.at[g], sib)
        copy(("b0", g), pdb.at[g, 1 - core], rbb.at[g], sib)

    def reduce_first(g):
        arrived(("a0", g), rba.at[g])
        arrived(("b0", g), rbb.at[g])
        rba[g] = (pda[g, core].astype(F32) + rba[g].astype(F32)).astype(BF)
        rbb[g] = (pdb[g, core].astype(F32) + rbb[g].astype(F32)).astype(BF)
        for d in (2, 1, 3):
            copy(("a1", g, d), rba.at[g, at(x + d)], ra.at[g, d - 1], dev(x + d, y, core))
            copy(("b1", g, d), rbb.at[g, at(y + d)], rb.at[g, d - 1], dev(x, y + d, core))

    def reduce_second(g):
        suma = rba[g, x].astype(F32)
        sumb = rbb[g, y].astype(F32)
        for d in (1, 3, 2):
            arrived(("a1", g, d), ra.at[g, d - 1])
            arrived(("b1", g, d), rb.at[g, d - 1])
            suma = suma + ra[g, d - 1].astype(F32)
            sumb = sumb + rb[g, d - 1].astype(F32)
        ua[g] = suma.astype(BF)
        ub[g] = sumb.astype(BF)
        for d in (2, 1, 3):
            copy(("a2", g, d), ua.at[g, at(y + d)], ra2.at[g, d - 1], dev(x, y + d, core))
            copy(("b2", g, d), ub.at[g, at(x + d)], rb2.at[g, d - 1], dev(x + d, y, core))

    def reduce_third(g):
        suma = ua[g, y].astype(F32)
        sumb = ub[g, x].astype(F32)
        for d in (1, 3, 2):
            arrived(("a2", g, d), ra2.at[g, d - 1])
            arrived(("b2", g, d), rb2.at[g, d - 1])
            suma = suma + ra2[g, d - 1].astype(F32)
            sumb = sumb + rb2[g, d - 1].astype(F32)
        dvf[g, :64] = suma.astype(BF)
        dvf[g, 64:] = sumb.astype(BF)
        copy(("r", g), dvf.at[g], dvr.at[g], prv)

    def slotted(first, held_n, mine, back):
        nothing = jnp.zeros_like(mine)
        carried = first + held_n > 1.5
        one = jnp.logical_and(carried, jnp.logical_and(held_n > 0.5, held_n < 1.5))
        both = jnp.logical_and(carried, held_n > 1.5)
        top = pick(first < 0.5, mine, pick(one, back, nothing))
        return top, pick(both, back, nothing)

    def grad_out(g):
        arrived(("r", g), dvr.at[g])
        kc = slice(g * D, (g + 1) * D)
        top, low = slotted(before, held_f, dvf[g], dvr[g])
        vgrad[:B, kc] = top
        vgrad[B:, kc] = low

    def hand_on(g):
        arrived(("h", g), hz.at[g])
        copy(("h2", g), hz.at[g], hr.at[g], prv)

    def hand_out(g):
        if g == 0:
            arrived("f", flr)
        arrived(("h2", g), hr.at[g])
        first, held_n = jnp.max(flr[0]), jnp.max(flr[1])
        for h in range(WIDE):
            hc = slice(h * D, (h + 1) * D)
            oc = slice(g * COLS + h * D, g * COLS + (h + 1) * D)
            top, low = slotted(first, held_n, hz[g, :, hc], hr[g, :, hc])
            handed[:B, oc] = top
            handed[B:, oc] = low

    def gate_out():
        gate_row = gr[...]
        total = jnp.sum(att_acc[1].T, axis=0, keepdims=True)
        ls_row = gate_row * (1.0 - gate_row) * jnp.broadcast_to(total, (8, 128))
        gs[0] = ls_row
        copy("g", gs.at[0], gs.at[1], prv)

    for g in range(GROUPS):
        gather_second(g)
    gather_third(0)
    gather_third(1)
    gather_fourth(0)
    gather_last(0)
    for g in range(GROUPS):
        forward(g)
        if g + 2 < GROUPS:
            gather_third(g + 2)
        if g + 1 < GROUPS:
            gather_fourth(g + 1)
        if g >= 1:
            reduce_second(g - 1)
            hand_on(g - 1)
        backward(g)
        if g == GROUPS - 1:
            gate_out()
        if g + 1 < GROUPS:
            gather_last(g + 1)
        reduce_first(g)
        if g >= 1:
            reduce_third(g - 1)
            hand_out(g - 1)
        if g >= 2:
            grad_out(g - 2)
    last = GROUPS - 1
    hand_on(last)
    reduce_second(last)
    grad_out(last - 1)
    hand_out(last)
    reduce_third(last)
    arrived("g", gs.at[1])
    top, low = slotted(before, held_f, gs[0, :1], gs[1, :1])
    ggrad[:, :B] = top.astype(BF)
    ggrad[:, B:] = low.astype(BF)
    grad_out(last)

    every.wait_send()
    for one in made:
        one.wait_send()


def local(queries, keys, values, cotangent, router_logits, positions, counts):
    del positions
    V = pl.BlockSpec(memory_space=pltpu.VMEM)
    G = GROUPS
    vm = pltpu.VMEM
    scratch = [
        vm((CTX, 8, 128), jnp.int32),
        vm((G, B, COLS), BF), vm((G, B, COLS), BF), vm((G, B, COLS), BF), vm((G, B, COLS), BF),
        vm((G, B, D), BF), vm((G, B, D), BF), vm((G, B, D), BF), vm((G, B, D), BF),
        vm((8, 128), F32), vm((8, 128), F32), vm((2, 8, 128), F32), vm((8, 128), F32),
        vm((2, 8, 128), F32), vm((2, 8, 128), F32),
        vm((G, 2, 4, 4, B, D), BF), vm((G, 2, 4, 4, B, D), BF),
        vm((CTX * B, COLS), F32), vm((CTX * B, COLS), BF),
        vm((2 * D, COLS), BF), vm((D + 16, COLS), F32), vm((COLS, D), BF), vm((2, B, D), F32),
        vm((G, 2, 4, 4, 64, D), BF), vm((G, 2, 4, 4, 64, D), BF),
        vm((G, 4, 4, 64, D), BF), vm((G, 4, 4, 64, D), BF),
        vm((G, 3, 4, 64, D), BF), vm((G, 3, 4, 64, D), BF),
        vm((G, 4, 64, D), BF), vm((G, 4, 64, D), BF),
        vm((G, 3, 64, D), BF), vm((G, 3, 64, D), BF),
        vm((G, B, D), BF), vm((G, B, D), BF),
        vm((G, B, COLS), BF), vm((G, B, COLS), BF), vm((G, B, COLS), BF),
        pltpu.SemaphoreType.DMA((2,)),
        pltpu.SemaphoreType.DMA((NCOPY,)),
        pltpu.SemaphoreType.DMA((NCOPY,)),
    ]
    handed, vgrad, ggrad = pl.pallas_call(
        kernel,
        out_shape=(
            jax.ShapeDtypeStruct((2 * B, G * COLS), BF),
            jax.ShapeDtypeStruct((2 * B, G * D), BF),
            jax.ShapeDtypeStruct((1, 2 * B), BF),
        ),
        in_specs=[pl.BlockSpec(memory_space=pltpu.SMEM)] + [V] * 5,
        out_specs=(V, V, V),
        scratch_shapes=scratch,
        compiler_params=pltpu.CompilerParams(
            collective_id=0, has_side_effects=True, vmem_limit_bytes=66_000_000
        ),
        name="routed_block",
    )(counts, queries[0], keys[0], values[0], cotangent[0], router_logits)
    return handed[None], vgrad[None], ggrad


def solution(mesh):
    return jax.shard_map(
        local,
        mesh=mesh,
        in_specs=(
            P("section", "ctx", None),
            P("section", "ctx", None),
            P("section", "ctx", None),
            P("section", "ctx", None),
            P("section", "ctx"),
            P("section", "ctx"),
            P("section", "ctx"),
        ),
        out_specs=(P("section", "ctx", None), P("section", "ctx", None), P("section", "ctx")),
        check_vma=False,
    )
```

```python
import math

import jax
import jax.numpy as jnp
from jax import lax
from jax.experimental import pallas as pl
from jax.experimental.pallas import tpu as pltpu
from jax.sharding import PartitionSpec as P

GROUPS = 4
WIDE = 6
D = 128
B = 128
COLS = WIDE * D
SECTIONS = 8
CTX = 32
TILE = 512
LOW = -1e30
SCALE = math.log2(math.e) / math.sqrt(D)
BF = jnp.bfloat16
F32 = jnp.float32
NCOPY = 260
DIRECT = False
Y_LARGE = (0, 1, 2, 3)


def kernel(
    counts, q_in, k_in, v_in, ct_in, lg_in,
    hz, hr, dvf, dvr, gs, fl, flr,
    cb, qs, qr, cs, cr, ks, kr, vs, vr, ls, lr, gr,
    kb, vb, sbuf, wbuf, qt, ot, dos, att_acc,
    pda, pdb, rba, rbb, ra, rb, ua, ub, ra2, rb2,
    br, csem, send_sems, recv_sems,
):
    sec = lax.axis_index("section")
    c = lax.axis_index("ctx")
    core = lax.rem(c, 2)
    y = lax.rem(lax.div(c, 2), 4)
    x = lax.div(c, 8)

    def dev(xx, yy, kk):
        return (sec, (lax.rem(xx + 8, 4) * 4 + lax.rem(yy + 8, 4)) * 2 + kk)

    nxt = (sec, lax.rem(c + 1, CTX))
    prv = (sec, lax.rem(c + CTX - 1, CTX))
    zup = (lax.rem(sec + 1, SECTIONS), c)
    zdn = (lax.rem(sec + SECTIONS - 1, SECTIONS), c)
    sib = (sec, c + 1 - 2 * core)
    MESH = pl.DeviceIdType.MESH

    made = []
    slots = {}

    def copy(name, src, dst, to):
        n = slots.setdefault(name, len(slots))
        made.append(
            pltpu.make_async_remote_copy(
                src_ref=src, dst_ref=dst, send_sem=send_sems.at[n], recv_sem=recv_sems.at[n],
                device_id=to, device_id_type=MESH,
            )
        )
        made[-1].start()
        return made[-1]

    def arrived(name, dst):
        n = slots[name]
        pltpu.make_async_remote_copy(
            src_ref=dst, dst_ref=dst, send_sem=send_sems.at[n], recv_sem=recv_sems.at[n],
            device_id=sib, device_id_type=MESH,
        ).wait_recv()

    bar = pltpu.get_barrier_semaphore()

    @pl.loop(1, CTX)
    def _(d):
        pl.semaphore_signal(bar, inc=1, device_id=(sec, lax.rem(c + d, CTX)), device_id_type=MESH)

    pl.semaphore_signal(bar, inc=1, device_id=zup, device_id_type=MESH)
    pl.semaphore_signal(bar, inc=1, device_id=zdn, device_id_type=MESH)

    held = counts[0, 0]
    two = held == 2
    cb[pl.ds(c, 1)] = jnp.full((1, 1, 128), held, jnp.int32)

    def pick(flag, a, b):
        return lax.select(jnp.broadcast_to(flag, a.shape), a, b)

    for g in range(GROUPS):
        kc = slice(g * D, (g + 1) * D)
        qc = slice(g * COLS, (g + 1) * COLS)
        ks[g] = pick(two, k_in[B:, kc], k_in[:B, kc])
        vs[g] = pick(two, v_in[B:, kc], v_in[:B, kc])
        qs[g] = pick(two, q_in[B:, qc], q_in[:B, qc])
        cs[g] = pick(two, ct_in[B:, qc], ct_in[:B, qc])
    lg = lg_in[...].astype(F32)
    ls[...] = jnp.broadcast_to(pick(two, lg[:, B:], lg[:, :B]), (8, 128))

    pl.semaphore_wait(bar, CTX + 1)

    @pl.loop(1, CTX)
    def _(d):
        pltpu.make_async_remote_copy(
            src_ref=cb.at[c], dst_ref=cb.at[c], send_sem=csem.at[0], recv_sem=csem.at[1],
            device_id=(sec, lax.rem(c + d, CTX)), device_id_type=MESH,
        ).start()

    copy("k", ks, kr, nxt)
    copy("v", vs, vr, nxt)
    copy("l", ls, lr, nxt)

    every = pltpu.make_async_remote_copy(
        src_ref=cb.at[pl.ds(0, CTX - 1)], dst_ref=cb.at[pl.ds(0, CTX - 1)],
        send_sem=csem.at[0], recv_sem=csem.at[1], device_id=sib, device_id_type=MESH,
    )
    every.wait_recv()
    order = lax.broadcasted_iota(jnp.int32, (CTX, 1, 128), 0)
    ahead = jnp.sum(jnp.where(order < c, cb[...] - 1, 0), axis=0).astype(F32)
    before = jnp.max(ahead)
    late = before > 0.5
    held_f = held.astype(F32)
    fl[0] = jnp.broadcast_to(ahead, (8, 128))
    fl[1] = jnp.full((8, 128), held_f, F32)

    arrived("k", kr)
    arrived("v", vr)

    def at(v):
        return lax.rem(v + 8, 4)

    parts = {
        (kind, g): (kb if kind == "k" else vb, kind == "k" and g in Y_LARGE)
        for kind in ("k", "v")
        for g in range(GROUPS)
    }

    def place(kind, g):
        buf, y_large = parts[kind, g]
        small = (lambda d: dev(x + d, y, core)) if y_large else (lambda d: dev(x, y + d, core))
        large = (lambda d: dev(x, y + d, core)) if y_large else (lambda d: dev(x + d, y, core))
        return buf, y_large, (y, x) if y_large else (x, y), small, large

    def block(kind, g, kk, xx, yy):
        buf, y_large = parts[kind, g]
        return buf[g, kk, yy, xx] if y_large else buf[g, kk, xx, yy]

    for g in range(GROUPS):
        kc = slice(g * D, (g + 1) * D)
        for kind, got, own in (("k", kr, k_in), ("v", vr, v_in)):
            buf, _, (a, b), _, _ = place(kind, g)
            buf[g, core, a, b] = pick(late, got[g], own[:B, kc])
    copy("f", fl, flr, zup)

    def pass_on2(g):
        pass_on("q", g)
        pass_on("c", g)

    def gather_one(g):
        for kind in ("k", "v"):
            buf, _, (a, b), small, _ = place(kind, g)
            own = buf.at[g, core, a, b]
            for d in (1, 3, 2):
                copy((kind, 1, g, d), own, own, small(d))

    def gather_second(g):
        for kind in ("k", "v"):
            buf, _, (a, b), _, large = place(kind, g)
            for d in (1, 3, 2):
                arrived((kind, 1, g, d), buf.at[g, core, a, at(b - d)])
            own = buf.at[g, core, a]
            for d in (1, 3, 2) if DIRECT else (1, 3):
                copy((kind, 2, g, d), own, own, large(d))
            copy((kind, 4, g, 0), own, own, sib)

    def gather_third(g):
        for d in (1, 3):
            for kind in ("k", "v"):
                buf, _, (a, b), _, large = place(kind, g)
                aa = at(a - d)
                came = buf.at[g, core, aa]
                arrived((kind, 2, g, d), came)
                if not DIRECT:
                    half = buf.at[g, core, aa, pl.ds(d - 1, 2)]
                    copy((kind, 3, g, d), half, half, large(d))
                copy((kind, 4, g, d), came, came, sib)

    def gather_fourth(g):
        for kind in ("k", "v"):
            buf, _, (a, b), _, _ = place(kind, g)
            aa = at(a + 2)
            if DIRECT:
                arrived((kind, 2, g, 2), buf.at[g, core, aa])
            else:
                for d in (1, 3):
                    arrived((kind, 3, g, d), buf.at[g, core, aa, pl.ds(d - 1, 2)])
            copy((kind, 4, g, 2), buf.at[g, core, aa], buf.at[g, core, aa], sib)

    def gather_last(g):
        for kind in ("k", "v"):
            buf, _, (a, b), _, _ = place(kind, g)
            for d in (0, 1, 3, 2):
                arrived((kind, 4, g, d), buf.at[g, 1 - core, at(a - d)])

    def pass_on(name, g):
        if name == "q":
            copy(("q", g), qs.at[g], qr.at[g], nxt)
        else:
            copy(("c", g), cs.at[g], cr.at[g], nxt)

    tiles = lax.div(c, 4) + 1
    lane = lax.broadcasted_iota(jnp.int32, (TILE, 2 * D), 1)
    gap = lax.broadcasted_iota(jnp.int32, (TILE, 2 * D), 0) - lax.rem(lane, D)

    def forward(g, between, after):
        arrived(("q", g), qr.at[g])
        qc = slice(g * COLS, (g + 1) * COLS)
        for h in range(WIDE):
            hc = slice(h * D, (h + 1) * D)
            full = pick(late, qr[g, :, hc], q_in[:B, g * COLS + h * D : g * COLS + (h + 1) * D])
            full = (full.astype(F32) * SCALE).T
            high = full.astype(BF)
            qt[:D, hc] = high
            qt[D:, hc] = (full - high.astype(F32)).astype(BF)

        def scores(j, tops):
            xx, y0 = lax.div(j, 2), lax.rem(j, 2) * 2
            one = jnp.concatenate(
                [block("k", g, n % 2, xx, y0 + n // 2) for n in range(4)], axis=0
            )
            both = jnp.concatenate([one, one], axis=1)
            bound = c * B - j * TILE
            out = []
            for p in range(3):
                pc = slice(p * 2 * D, (p + 1) * 2 * D)
                s = jnp.dot(both, qt[:, pc], preferred_element_type=F32)
                s = jnp.where(gap <= bound, s, LOW)
                sbuf[pl.ds(pl.multiple_of(j * TILE, TILE), TILE), pc] = s
                out.append(jnp.maximum(tops[p], jnp.max(s.reshape(TILE // 8, 8, 2 * D), axis=0)))
            return tuple(out)

        tops = lax.fori_loop(
            0, tiles, scores, tuple(jnp.full((8, 2 * D), LOW, F32) for _ in range(3))
        )
        tops = [jnp.max(t, axis=0, keepdims=True) for t in tops]
        ot[...] = jnp.zeros_like(ot)
        between()

        def weigh(j, _):
            xx, y0 = lax.div(j, 2), lax.rem(j, 2) * 2
            one = jnp.concatenate(
                [block("v", g, n % 2, xx, y0 + n // 2) for n in range(4)], axis=0
            )
            left = jnp.concatenate([one.T, jnp.ones((16, TILE), BF)], axis=0)
            rows = pl.ds(pl.multiple_of(j * TILE, TILE), TILE)
            for p in range(3):
                pc = slice(p * 2 * D, (p + 1) * 2 * D)
                w = jnp.exp2(sbuf[rows, pc] - tops[p]).astype(BF)
                wbuf[rows, pc] = w
                ot[:, pc] += jnp.dot(left, w, preferred_element_type=F32)
            return 0

        lax.fori_loop(0, tiles, weigh, 0)
        after()
        if g == 0:
            arrived("l", lr)
            gate_row = 1.0 / (1.0 + jnp.exp(-pick(late, lr[...], jnp.broadcast_to(lg[:, :B], (8, 128)))))
            gr[...] = gate_row
            att_acc[0] = jnp.broadcast_to(gate_row[:1], (B, D)).T
            att_acc[1] = jnp.zeros((B, D), F32)
        arrived(("c", g), cr.at[g])
        gate = att_acc[0]
        acc = att_acc[1]
        for h in range(WIDE):
            hc = slice(h * D, (h + 1) * D)
            inv = 1.0 / ot[D : D + 1, hc]
            attended = (ot[:D, hc] * inv).T
            br[g, :, hc] = (gate * attended).astype(BF)
            ct = pick(late, cr[g, :, hc], ct_in[:B, g * COLS + h * D : g * COLS + (h + 1) * D]).astype(F32)
            acc = acc + ct * attended
            dos[hc, :] = (gate * ct * jnp.broadcast_to(inv, (B, D)).T).astype(BF)
        att_acc[1] = acc
        copy(("h", g), br.at[g], hz.at[:, g * COLS : (g + 1) * COLS], zup)

    def backward(g):
        def terms(j, _):
            xx, y0 = lax.div(j, 2), lax.rem(j, 2) * 2
            rows = pl.ds(pl.multiple_of(j * TILE, TILE), TILE)
            t = jnp.dot(wbuf[rows, :], dos[...], preferred_element_type=F32).astype(BF)
            for n in range(4):
                pda[g, n % 2, xx, y0 + n // 2] = t[n * B : n * B + 64]
                pdb[g, n % 2, y0 + n // 2, xx] = t[n * B + 64 : (n + 1) * B]
            return 0

        lax.fori_loop(0, tiles, terms, 0)

        def blank(j, _):
            xx, y0 = lax.div(j, 2), lax.rem(j, 2) * 2
            for n in range(4):
                pda[g, n % 2, xx, y0 + n // 2] = jnp.zeros((64, D), BF)
                pdb[g, n % 2, y0 + n // 2, xx] = jnp.zeros((64, D), BF)
            return 0

        lax.fori_loop(tiles, CTX // 4, blank, 0)
        copy(("a0", g), pda.at[g, 1 - core], rba.at[g], sib)
        copy(("b0", g), pdb.at[g, 1 - core], rbb.at[g], sib)

    def reduce_first(g):
        arrived(("a0", g), rba.at[g])
        arrived(("b0", g), rbb.at[g])
        rba[g] = (pda[g, core].astype(F32) + rba[g].astype(F32)).astype(BF)
        rbb[g] = (pdb[g, core].astype(F32) + rbb[g].astype(F32)).astype(BF)
        for d in (2, 1, 3):
            copy(("a1", g, d), rba.at[g, at(x + d)], ra.at[g, d - 1], dev(x + d, y, core))
            copy(("b1", g, d), rbb.at[g, at(y + d)], rb.at[g, d - 1], dev(x, y + d, core))

    def reduce_second(g):
        suma = rba[g, x].astype(F32)
        sumb = rbb[g, y].astype(F32)
        for d in (1, 3, 2):
            arrived(("a1", g, d), ra.at[g, d - 1])
            arrived(("b1", g, d), rb.at[g, d - 1])
            suma = suma + ra[g, d - 1].astype(F32)
            sumb = sumb + rb[g, d - 1].astype(F32)
        ua[g] = suma.astype(BF)
        ub[g] = sumb.astype(BF)
        for d in (2, 1, 3):
            copy(("a2", g, d), ua.at[g, at(y + d)], ra2.at[g, d - 1], dev(x, y + d, core))
            copy(("b2", g, d), ub.at[g, at(x + d)], rb2.at[g, d - 1], dev(x + d, y, core))

    def reduce_third(g):
        suma = ua[g, y].astype(F32)
        sumb = ub[g, x].astype(F32)
        for d in (1, 3, 2):
            arrived(("a2", g, d), ra2.at[g, d - 1])
            arrived(("b2", g, d), rb2.at[g, d - 1])
            suma = suma + ra2[g, d - 1].astype(F32)
            sumb = sumb + rb2[g, d - 1].astype(F32)
        kc = slice(g * D, (g + 1) * D)
        dvf[:64, kc] = suma.astype(BF)
        dvf[64:, kc] = sumb.astype(BF)
        copy(("r", g), dvf.at[:, kc], dvr.at[:, kc], prv)

    def hand_on(g):
        oc = slice(g * COLS, (g + 1) * COLS)
        arrived(("h", g), hz.at[:, oc])
        copy(("h2", g), hz.at[:, oc], hr.at[:, oc], prv)

    def gate_out():
        gate_row = gr[...]
        total = jnp.sum(att_acc[1].T, axis=0, keepdims=True)
        ls_row = gate_row * (1.0 - gate_row) * jnp.broadcast_to(total, (8, 128))
        gs[0] = ls_row
        copy("g", gs.at[0], gs.at[1], prv)

    for g in range(GROUPS):
        gather_one(g)
    pass_on("q", 0)
    gather_second(0)
    gather_second(1)
    pass_on("c", 0)
    gather_third(0)
    gather_second(2)
    gather_fourth(0)
    gather_second(3)
    pass_on("q", 1)
    gather_third(1)
    gather_last(0)
    pass_on("c", 1)
    plan = {
        (0, 0): [(pass_on2, 2), (gather_third, 2)],
        (0, 1): [(gather_fourth, 1)],
        (0, 2): [(gather_third, 3), (pass_on2, 3)],
        (0, 3): [(gather_last, 1), (gather_fourth, 2)],
        (1, 0): [(reduce_first, 0)],
        (1, 1): [(hand_on, 0), (gather_fourth, 3)],
        (1, 2): [(gather_last, 2)],
        (1, 3): [(reduce_second, 0)],
        (2, 0): [(reduce_first, 1)],
        (2, 1): [(reduce_third, 0), (hand_on, 1)],
        (2, 2): [(gather_last, 3)],
        (2, 3): [(reduce_second, 1)],
        (3, 0): [(reduce_first, 2)],
        (3, 1): [(reduce_third, 1), (hand_on, 2)],
        (3, 2): [(reduce_second, 2)],
        (3, 3): [],
    }
    for g in range(GROUPS):
        def at_slot(n):
            for what, k in plan[g, n]:
                what(k)

        forward(g, lambda: at_slot(0), lambda: at_slot(1))
        at_slot(2)
        backward(g)
        if g == GROUPS - 1:
            gate_out()
        at_slot(3)
    last = GROUPS - 1
    reduce_first(last)
    reduce_third(2)
    reduce_second(last)
    hand_on(last)
    reduce_third(last)
    arrived("f", flr)
    arrived("g", gs.at[1])
    for g in range(GROUPS):
        arrived(("h2", g), hr.at[:, g * COLS : (g + 1) * COLS])
        arrived(("r", g), dvr.at[:, g * D : (g + 1) * D])

    every.wait_send()
    for one in made:
        one.wait_send()


def finish(hz, hr, dvf, dvr, gs, fl, flr, handed, vgrad, ggrad):
    def slotted(flags, mine, back, out, cols):
        first, held = jnp.max(flags[0]), jnp.max(flags[1])
        carried = first + held > 1.5
        one = jnp.logical_and(carried, jnp.logical_and(held > 0.5, held < 1.5))
        both = jnp.logical_and(carried, held > 1.5)
        nothing = jnp.zeros_like(mine)

        def pick(flag, a, b):
            return lax.select(jnp.broadcast_to(flag, a.shape), a, b)

        out(pick(first < 0.5, mine, pick(one, back, nothing)), pick(both, back, nothing), cols)

    def rows(ref):
        def put(top, low, cols):
            ref[:B, cols] = top
            ref[B:, cols] = low

        return put

    def lanes(top, low, cols):
        ggrad[:, :B] = top.astype(BF)
        ggrad[:, B:] = low.astype(BF)

    for n in range(GROUPS * WIDE):
        cols = slice(n * D, (n + 1) * D)
        slotted(flr, hz[:, cols], hr[:, cols], rows(handed), cols)
    for n in range(GROUPS):
        cols = slice(n * D, (n + 1) * D)
        slotted(fl, dvf[:, cols], dvr[:, cols], rows(vgrad), cols)
    slotted(fl, gs[0, :1], gs[1, :1], lanes, None)


def local(queries, keys, values, cotangent, router_logits, positions, counts):
    del positions
    V = pl.BlockSpec(memory_space=pltpu.VMEM)
    G = GROUPS
    vm = pltpu.VMEM
    scratch = [
        vm((CTX, 1, 128), jnp.int32),
        vm((G, B, COLS), BF), vm((G, B, COLS), BF), vm((G, B, COLS), BF), vm((G, B, COLS), BF),
        vm((G, B, D), BF), vm((G, B, D), BF), vm((G, B, D), BF), vm((G, B, D), BF),
        vm((8, 128), F32), vm((8, 128), F32), vm((8, 128), F32),
        vm((G, 2, 4, 4, B, D), BF), vm((G, 2, 4, 4, B, D), BF),
        vm((CTX * B, COLS), F32), vm((CTX * B, COLS), BF),
        vm((2 * D, COLS), BF), vm((D + 16, COLS), F32), vm((COLS, D), BF), vm((2, B, D), F32),
        vm((G, 2, 4, 4, 64, D), BF), vm((G, 2, 4, 4, 64, D), BF),
        vm((G, 4, 4, 64, D), BF), vm((G, 4, 4, 64, D), BF),
        vm((G, 3, 4, 64, D), BF), vm((G, 3, 4, 64, D), BF),
        vm((G, 4, 64, D), BF), vm((G, 4, 64, D), BF),
        vm((G, 3, 64, D), BF), vm((G, 3, 64, D), BF),
        vm((G, B, COLS), BF),
        pltpu.SemaphoreType.DMA((2,)),
        pltpu.SemaphoreType.DMA((NCOPY,)),
        pltpu.SemaphoreType.DMA((NCOPY,)),
    ]
    hz, hr, dvf, dvr, gs, fl, flr = pl.pallas_call(
        kernel,
        out_shape=(
            jax.ShapeDtypeStruct((B, G * COLS), BF),
            jax.ShapeDtypeStruct((B, G * COLS), BF),
            jax.ShapeDtypeStruct((B, G * D), BF),
            jax.ShapeDtypeStruct((B, G * D), BF),
            jax.ShapeDtypeStruct((2, 8, 128), F32),
            jax.ShapeDtypeStruct((2, 8, 128), F32),
            jax.ShapeDtypeStruct((2, 8, 128), F32),
        ),
        in_specs=[pl.BlockSpec(memory_space=pltpu.SMEM)] + [V] * 5,
        out_specs=(V,) * 7,
        scratch_shapes=scratch,
        compiler_params=pltpu.CompilerParams(
            collective_id=0, has_side_effects=True, vmem_limit_bytes=66_000_000
        ),
        name="routed_block",
    )(counts, queries[0], keys[0], values[0], cotangent[0], router_logits)
    handed, vgrad, ggrad = pl.pallas_call(
        finish,
        out_shape=(
            jax.ShapeDtypeStruct((2 * B, G * COLS), BF),
            jax.ShapeDtypeStruct((2 * B, G * D), BF),
            jax.ShapeDtypeStruct((1, 2 * B), BF),
        ),
        in_specs=[V] * 7,
        out_specs=(V, V, V),
        name="slots",
    )(hz, hr, dvf, dvr, gs, fl, flr)
    return handed[None], vgrad[None], ggrad


def solution(mesh):
    return jax.shard_map(
        local,
        mesh=mesh,
        in_specs=(
            P("section", "ctx", None),
            P("section", "ctx", None),
            P("section", "ctx", None),
            P("section", "ctx", None),
            P("section", "ctx"),
            P("section", "ctx"),
            P("section", "ctx"),
        ),
        out_specs=(P("section", "ctx", None), P("section", "ctx", None), P("section", "ctx")),
        check_vma=False,
    )
```

```python
import math

import jax
import jax.numpy as jnp
from jax import lax
from jax.experimental import pallas as pl
from jax.experimental.pallas import tpu as pltpu
from jax.sharding import PartitionSpec as P

GROUPS = 4
WIDE = 6
D = 128
B = 128
COLS = WIDE * D
SECTIONS = 8
CTX = 32
TILE = 2048
NB = TILE // B
LOW = -1e30
SCALE = math.log2(math.e) / math.sqrt(D)
BF = jnp.bfloat16
F32 = jnp.float32
NCOPY = 57
DIRECT = (0,)
Y_LARGE = (0, 1, 2, 3)


def kernel(
    counts, q_in, k_in, v_in, ct_in, lg_in,
    hz, hr, dvf, dvr, gs, fl, flr,
    cb, qs, qr, cs, cr, ks, kr, vs, vr, ls, lr, gr,
    kb, vb, sbuf, wbuf, qt, ot, dos, att_acc,
    pda, pdb, rba, rbb, ra, rb, ua, ub, ra2, rb2,
    br, csem, send_sems, recv_sems,
):
    sec = lax.axis_index("section")
    c = lax.axis_index("ctx")
    core = lax.rem(c, 2)
    y = lax.rem(lax.div(c, 2), 4)
    x = lax.div(c, 8)

    def dev(xx, yy, kk):
        return (sec, (lax.rem(xx + 8, 4) * 4 + lax.rem(yy + 8, 4)) * 2 + kk)

    nxt = (sec, lax.rem(c + 1, CTX))
    prv = (sec, lax.rem(c + CTX - 1, CTX))
    zup = (lax.rem(sec + 1, SECTIONS), c)
    zdn = (lax.rem(sec + SECTIONS - 1, SECTIONS), c)
    sib = (sec, c + 1 - 2 * core)
    MESH = pl.DeviceIdType.MESH

    sets = {
        "s1": kb.at[0, 0, pl.ds(0, 2), pl.ds(0, 3)],
        "s2": kb.at[0, 0, pl.ds(0, 2)],
        "s3": kb.at[0, 0, pl.ds(0, 2)],
        "s4": kb.at[0],
        "a0": pda.at[0],
        "a1": pda.at[0, pl.ds(0, 2), pl.ds(0, 3)],
        "a3": pda.at[0, 0, pl.ds(0, 2), pl.ds(0, 3)],
    }
    slots = {}

    def copy(name, src, dst, to):
        n, _ = slots.setdefault(name, (len(slots), sets.get(name[0], dst)))
        pltpu.make_async_remote_copy(
            src_ref=src, dst_ref=dst, send_sem=send_sems.at[n], recv_sem=recv_sems.at[n],
            device_id=to, device_id_type=MESH,
        ).start()

    def whole(name):
        n, ref = slots[name]
        return pltpu.make_async_remote_copy(
            src_ref=ref, dst_ref=ref, send_sem=send_sems.at[n], recv_sem=recv_sems.at[n],
            device_id=sib, device_id_type=MESH,
        )

    def arrived(*name):
        whole(name).wait_recv()

    bar = pltpu.get_barrier_semaphore()

    @pl.loop(1, CTX)
    def _(d):
        pl.semaphore_signal(bar, inc=1, device_id=(sec, lax.rem(c + d, CTX)), device_id_type=MESH)

    pl.semaphore_signal(bar, inc=1, device_id=zup, device_id_type=MESH)
    pl.semaphore_signal(bar, inc=1, device_id=zdn, device_id_type=MESH)

    held = counts[0, 0]
    two = held == 2
    cb[pl.ds(c, 1)] = jnp.full((1, 1, 128), held, jnp.int32)

    def pick(flag, a, b):
        return lax.select(jnp.broadcast_to(flag, a.shape), a, b)

    for g in range(GROUPS):
        kc = slice(g * D, (g + 1) * D)
        qc = slice(g * COLS, (g + 1) * COLS)
        ks[g] = pick(two, k_in[B:, kc], k_in[:B, kc])
        vs[g] = pick(two, v_in[B:, kc], v_in[:B, kc])
        qs[g] = pick(two, q_in[B:, qc], q_in[:B, qc])
        cs[g] = pick(two, ct_in[B:, qc], ct_in[:B, qc])
    lg = lg_in[...].astype(F32)
    ls[...] = jnp.broadcast_to(pick(two, lg[:, B:], lg[:, :B]), (8, 128))

    pl.semaphore_wait(bar, CTX + 1)

    @pl.loop(1, CTX)
    def _(d):
        pltpu.make_async_remote_copy(
            src_ref=cb.at[c], dst_ref=cb.at[c], send_sem=csem.at[0], recv_sem=csem.at[1],
            device_id=(sec, lax.rem(c + d, CTX)), device_id_type=MESH,
        ).start()

    copy(("k",), ks, kr, nxt)
    copy(("v",), vs, vr, nxt)
    copy(("l",), ls, lr, nxt)
    copy(("q", 0), qs.at[0], qr.at[0], nxt)

    every = pltpu.make_async_remote_copy(
        src_ref=cb.at[pl.ds(0, CTX - 1)], dst_ref=cb.at[pl.ds(0, CTX - 1)],
        send_sem=csem.at[0], recv_sem=csem.at[1], device_id=sib, device_id_type=MESH,
    )
    every.wait_recv()
    order = lax.broadcasted_iota(jnp.int32, (CTX, 1, 128), 0)
    ahead = jnp.sum(jnp.where(order < c, cb[...] - 1, 0), axis=0).astype(F32)
    before = jnp.max(ahead)
    late = before > 0.5
    held_f = held.astype(F32)
    fl[0] = jnp.broadcast_to(ahead, (8, 128))
    fl[1] = jnp.full((8, 128), held_f, F32)

    arrived("k")
    arrived("v")

    def at(v):
        return lax.rem(v + 8, 4)

    parts = {
        (kind, g): (kb if kind == "k" else vb, kind == "k" and g in Y_LARGE)
        for kind in ("k", "v")
        for g in range(GROUPS)
    }

    def place(kind, g):
        buf, y_large = parts[kind, g]
        small = (lambda d: dev(x + d, y, core)) if y_large else (lambda d: dev(x, y + d, core))
        large = (lambda d: dev(x, y + d, core)) if y_large else (lambda d: dev(x + d, y, core))
        return buf, y_large, (y, x) if y_large else (x, y), small, large

    def block(kind, g, kk, xx, yy):
        buf, y_large = parts[kind, g]
        return buf[g, kk, yy, xx] if y_large else buf[g, kk, xx, yy]

    for g in range(GROUPS):
        kc = slice(g * D, (g + 1) * D)
        for kind, got, own in (("k", kr, k_in), ("v", vr, v_in)):
            buf, _, (a, b), _, _ = place(kind, g)
            buf[g, core, a, b] = pick(late, got[g], own[:B, kc])
    copy(("f",), fl, flr, zup)

    def pass_q(g):
        pass_on("q", g)

    def pass_c(g):
        pass_on("c", g)

    def gather_one(g):
        for kind in ("k", "v"):
            buf, _, (a, b), small, _ = place(kind, g)
            own = buf.at[g, core, a, b]
            for d in (1, 3, 2):
                copy(("s1", g), own, own, small(d))

    def gather_second(g):
        arrived("s1", g)
        for d in (1, 3, 2) if g in DIRECT else (1, 3):
            for kind in ("k", "v"):
                buf, _, (a, b), _, large = place(kind, g)
                own = buf.at[g, core, a]
                copy(("s2", g, d), own, own, large(d))
        for kind in ("k", "v"):
            buf, _, (a, b), _, _ = place(kind, g)
            copy(("s4", g), buf.at[g, core, a], buf.at[g, core, a], sib)

    def gather_third(g):
        for d in (1, 3):
            arrived("s2", g, d)
            for kind in ("k", "v"):
                buf, _, (a, b), _, large = place(kind, g)
                aa = at(a - d)
                came = buf.at[g, core, aa]
                if g not in DIRECT:
                    half = buf.at[g, core, aa, pl.ds(d - 1, 2)]
                    copy(("s3", g), half, half, large(d))
                copy(("s4", g), came, came, sib)

    def gather_fourth(g):
        if g in DIRECT:
            arrived("s2", g, 2)
        else:
            arrived("s3", g)
        for kind in ("k", "v"):
            buf, _, (a, b), _, _ = place(kind, g)
            aa = at(a + 2)
            copy(("s4", g), buf.at[g, core, aa], buf.at[g, core, aa], sib)

    def gather_last(g):
        arrived("s4", g)

    def pass_on(name, g):
        if name == "q":
            copy(("q", g), qs.at[g], qr.at[g], nxt)
        else:
            copy(("c", g), cs.at[g], cr.at[g], nxt)

    tiles = lax.div(c, NB) + 1
    lane = lax.broadcasted_iota(jnp.int32, (TILE, 2 * D), 1)
    gap = lax.broadcasted_iota(jnp.int32, (TILE, 2 * D), 0) - lax.rem(lane, D)

    def forward(g, between, after):
        arrived("q", g)
        qc = slice(g * COLS, (g + 1) * COLS)
        for h in range(WIDE):
            hc = slice(h * D, (h + 1) * D)
            full = pick(late, qr[g, :, hc], q_in[:B, g * COLS + h * D : g * COLS + (h + 1) * D])
            full = (full.astype(F32) * SCALE).T
            high = full.astype(BF)
            qt[:D, hc] = high
            qt[D:, hc] = (full - high.astype(F32)).astype(BF)

        def scores(j, tops):
            xx = j * 2
            one = jnp.concatenate(
                [block("k", g, n % 2, xx + n // 8, n % 8 // 2) for n in range(NB)], axis=0
            )
            both = jnp.concatenate([one, one], axis=1)
            bound = c * B - j * TILE
            out = []
            for p in range(3):
                pc = slice(p * 2 * D, (p + 1) * 2 * D)
                s = jnp.dot(both, qt[:, pc], preferred_element_type=F32)
                s = jnp.where(gap <= bound, s, LOW)
                sbuf[pl.ds(pl.multiple_of(j * TILE, TILE), TILE), pc] = s
                out.append(jnp.maximum(tops[p], jnp.max(s.reshape(TILE // 8, 8, 2 * D), axis=0)))
            return tuple(out)

        tops = lax.fori_loop(
            0, tiles, scores, tuple(jnp.full((8, 2 * D), LOW, F32) for _ in range(3))
        )
        tops = [jnp.max(t, axis=0, keepdims=True) for t in tops]
        ot[...] = jnp.zeros_like(ot)
        between()

        def weigh(j, _):
            xx = j * 2
            one = jnp.concatenate(
                [block("v", g, n % 2, xx + n // 8, n % 8 // 2) for n in range(NB)], axis=0
            )
            left = jnp.concatenate([one.T, jnp.ones((16, TILE), BF)], axis=0)
            rows = pl.ds(pl.multiple_of(j * TILE, TILE), TILE)
            for p in range(3):
                pc = slice(p * 2 * D, (p + 1) * 2 * D)
                w = jnp.exp2(sbuf[rows, pc] - tops[p]).astype(BF)
                wbuf[rows, pc] = w
                ot[:, pc] += jnp.dot(left, w, preferred_element_type=F32)
            return 0

        lax.fori_loop(0, tiles, weigh, 0)
        after()
        if g == 0:
            arrived("l")
            gate_row = 1.0 / (1.0 + jnp.exp(-pick(late, lr[...], jnp.broadcast_to(lg[:, :B], (8, 128)))))
            gr[...] = gate_row
            att_acc[0] = jnp.broadcast_to(gate_row[:1], (B, D)).T
            att_acc[1] = jnp.zeros((B, D), F32)
        arrived("c", g)
        gate = att_acc[0]
        acc = att_acc[1]
        for h in range(WIDE):
            hc = slice(h * D, (h + 1) * D)
            inv = 1.0 / ot[D : D + 1, hc]
            attended = (ot[:D, hc] * inv).T
            br[g, :, hc] = (gate * attended).astype(BF)
            ct = pick(late, cr[g, :, hc], ct_in[:B, g * COLS + h * D : g * COLS + (h + 1) * D]).astype(F32)
            acc = acc + ct * attended
            dos[hc, :] = (gate * ct * jnp.broadcast_to(inv, (B, D)).T).astype(BF)
        att_acc[1] = acc
        copy(("h", g), br.at[g], hz.at[:, g * COLS : (g + 1) * COLS], zup)

    def backward(g):
        def terms(j, _):
            xx = j * 2
            rows = pl.ds(pl.multiple_of(j * TILE, TILE), TILE)
            t = jnp.dot(wbuf[rows, :], dos[...], preferred_element_type=F32).astype(BF)
            for n in range(NB):
                pda[g, n % 2, xx + n // 8, n % 8 // 2] = t[n * B : n * B + 64]
                pdb[g, n % 2, n % 8 // 2, xx + n // 8] = t[n * B + 64 : (n + 1) * B]
            return 0

        lax.fori_loop(0, tiles, terms, 0)

        def blank(j, _):
            xx = j * 2
            for n in range(NB):
                pda[g, n % 2, xx + n // 8, n % 8 // 2] = jnp.zeros((64, D), BF)
                pdb[g, n % 2, n % 8 // 2, xx + n // 8] = jnp.zeros((64, D), BF)
            return 0

        lax.fori_loop(tiles, CTX // NB, blank, 0)
        copy(("a0", g), pda.at[g, 1 - core], rba.at[g], sib)
        copy(("a0", g), pdb.at[g, 1 - core], rbb.at[g], sib)

    def reduce_first(g):
        arrived("a0", g)
        rba[g] = (pda[g, core].astype(F32) + rba[g].astype(F32)).astype(BF)
        rbb[g] = (pdb[g, core].astype(F32) + rbb[g].astype(F32)).astype(BF)
        for d in (2, 1, 3):
            copy(("a1", g), rba.at[g, at(x + d)], ra.at[g, d - 1], dev(x + d, y, core))
            copy(("a1", g), rbb.at[g, at(y + d)], rb.at[g, d - 1], dev(x, y + d, core))

    def reduce_second(g):
        suma = rba[g, x].astype(F32)
        sumb = rbb[g, y].astype(F32)
        arrived("a1", g)
        for d in (1, 3, 2):
            suma = suma + ra[g, d - 1].astype(F32)
            sumb = sumb + rb[g, d - 1].astype(F32)
        ua[g] = suma.astype(BF)
        ub[g] = sumb.astype(BF)
        for d in (2, 1, 3):
            copy(("a3", g), ua.at[g, at(y + d)], ra2.at[g, d - 1], dev(x, y + d, core))
            copy(("a3", g), ub.at[g, at(x + d)], rb2.at[g, d - 1], dev(x + d, y, core))

    def reduce_third(g):
        suma = ua[g, y].astype(F32)
        sumb = ub[g, x].astype(F32)
        arrived("a3", g)
        for d in (1, 3, 2):
            suma = suma + ra2[g, d - 1].astype(F32)
            sumb = sumb + rb2[g, d - 1].astype(F32)
        kc = slice(g * D, (g + 1) * D)
        dvf[:64, kc] = suma.astype(BF)
        dvf[64:, kc] = sumb.astype(BF)
        copy(("r", g), dvf.at[:, kc], dvr.at[:, kc], prv)

    def hand_on(g):
        oc = slice(g * COLS, (g + 1) * COLS)
        arrived("h", g)
        copy(("h2", g), hz.at[:, oc], hr.at[:, oc], prv)

    def gate_out():
        gate_row = gr[...]
        total = jnp.sum(att_acc[1].T, axis=0, keepdims=True)
        ls_row = gate_row * (1.0 - gate_row) * jnp.broadcast_to(total, (8, 128))
        gs[0] = ls_row
        copy(("g",), gs.at[0], gs.at[1], prv)

    gather_one(0)
    gather_second(0)
    gather_one(1)
    gather_third(0)
    gather_one(2)
    gather_second(1)
    pass_on("c", 0)
    gather_fourth(0)
    gather_one(3)
    gather_last(0)
    plan = {
        (0, 0): [(gather_third, 1), (gather_second, 2), (pass_q, 1)],
        (0, 1): [(pass_c, 1)],
        (0, 2): [(gather_fourth, 1), (gather_second, 3)],
        (0, 3): [(gather_third, 2), (gather_last, 1), (pass_q, 2), (pass_c, 2)],
        (1, 0): [(reduce_first, 0)],
        (1, 1): [(gather_third, 3), (hand_on, 0)],
        (1, 2): [(gather_fourth, 2), (pass_q, 3), (pass_c, 3)],
        (1, 3): [(reduce_second, 0), (gather_last, 2)],
        (2, 0): [(reduce_first, 1), (gather_fourth, 3)],
        (2, 1): [(reduce_third, 0), (hand_on, 1)],
        (2, 2): [(gather_last, 3)],
        (2, 3): [(reduce_second, 1)],
        (3, 0): [(reduce_first, 2)],
        (3, 1): [(reduce_third, 1), (hand_on, 2)],
        (3, 2): [(reduce_second, 2)],
        (3, 3): [],
    }
    for g in range(GROUPS):
        def at_slot(n):
            for what, k in plan[g, n]:
                what(k)

        forward(g, lambda: at_slot(0), lambda: at_slot(1))
        at_slot(2)
        backward(g)
        if g == GROUPS - 1:
            gate_out()
        at_slot(3)
    last = GROUPS - 1
    reduce_first(last)
    reduce_third(2)
    hand_on(last)
    reduce_second(last)
    reduce_third(last)
    arrived("f")
    arrived("g")
    for g in range(GROUPS):
        arrived("h2", g)
        arrived("r", g)

    every.wait_send()
    for name in slots:
        whole(name).wait_send()


def finish(hz, hr, dvf, dvr, gs, fl, flr, handed, vgrad, ggrad):
    def slotted(flags, mine, back, out, cols):
        first, held = jnp.max(flags[0]), jnp.max(flags[1])
        carried = first + held > 1.5
        one = jnp.logical_and(carried, jnp.logical_and(held > 0.5, held < 1.5))
        both = jnp.logical_and(carried, held > 1.5)
        nothing = jnp.zeros_like(mine)

        def pick(flag, a, b):
            return lax.select(jnp.broadcast_to(flag, a.shape), a, b)

        out(pick(first < 0.5, mine, pick(one, back, nothing)), pick(both, back, nothing), cols)

    def rows(ref):
        def put(top, low, cols):
            ref[:B, cols] = top
            ref[B:, cols] = low

        return put

    def lanes(top, low, cols):
        ggrad[:, :B] = top.astype(BF)
        ggrad[:, B:] = low.astype(BF)

    for n in range(GROUPS * WIDE):
        cols = slice(n * D, (n + 1) * D)
        slotted(flr, hz[:, cols], hr[:, cols], rows(handed), cols)
    for n in range(GROUPS):
        cols = slice(n * D, (n + 1) * D)
        slotted(fl, dvf[:, cols], dvr[:, cols], rows(vgrad), cols)
    slotted(fl, gs[0, :1], gs[1, :1], lanes, None)


def local(queries, keys, values, cotangent, router_logits, positions, counts):
    del positions
    V = pl.BlockSpec(memory_space=pltpu.VMEM)
    G = GROUPS
    vm = pltpu.VMEM
    scratch = [
        vm((CTX, 1, 128), jnp.int32),
        vm((G, B, COLS), BF), vm((G, B, COLS), BF), vm((G, B, COLS), BF), vm((G, B, COLS), BF),
        vm((G, B, D), BF), vm((G, B, D), BF), vm((G, B, D), BF), vm((G, B, D), BF),
        vm((8, 128), F32), vm((8, 128), F32), vm((8, 128), F32),
        vm((G, 2, 4, 4, B, D), BF), vm((G, 2, 4, 4, B, D), BF),
        vm((CTX * B, COLS), F32), vm((CTX * B, COLS), BF),
        vm((2 * D, COLS), BF), vm((D + 16, COLS), F32), vm((COLS, D), BF), vm((2, B, D), F32),
        vm((G, 2, 4, 4, 64, D), BF), vm((G, 2, 4, 4, 64, D), BF),
        vm((G, 4, 4, 64, D), BF), vm((G, 4, 4, 64, D), BF),
        vm((G, 3, 4, 64, D), BF), vm((G, 3, 4, 64, D), BF),
        vm((G, 4, 64, D), BF), vm((G, 4, 64, D), BF),
        vm((G, 3, 64, D), BF), vm((G, 3, 64, D), BF),
        vm((G, B, COLS), BF),
        pltpu.SemaphoreType.DMA((2,)),
        pltpu.SemaphoreType.DMA((NCOPY,)),
        pltpu.SemaphoreType.DMA((NCOPY,)),
    ]
    hz, hr, dvf, dvr, gs, fl, flr = pl.pallas_call(
        kernel,
        out_shape=(
            jax.ShapeDtypeStruct((B, G * COLS), BF),
            jax.ShapeDtypeStruct((B, G * COLS), BF),
            jax.ShapeDtypeStruct((B, G * D), BF),
            jax.ShapeDtypeStruct((B, G * D), BF),
            jax.ShapeDtypeStruct((2, 8, 128), F32),
            jax.ShapeDtypeStruct((2, 8, 128), F32),
            jax.ShapeDtypeStruct((2, 8, 128), F32),
        ),
        in_specs=[pl.BlockSpec(memory_space=pltpu.SMEM)] + [V] * 5,
        out_specs=(V,) * 7,
        scratch_shapes=scratch,
        compiler_params=pltpu.CompilerParams(
            collective_id=0, has_side_effects=True, vmem_limit_bytes=66_000_000
        ),
        name="routed_block",
    )(counts, queries[0], keys[0], values[0], cotangent[0], router_logits)
    handed, vgrad, ggrad = pl.pallas_call(
        finish,
        out_shape=(
            jax.ShapeDtypeStruct((2 * B, G * COLS), BF),
            jax.ShapeDtypeStruct((2 * B, G * D), BF),
            jax.ShapeDtypeStruct((1, 2 * B), BF),
        ),
        in_specs=[V] * 7,
        out_specs=(V, V, V),
        name="slots",
    )(hz, hr, dvf, dvr, gs, fl, flr)
    return handed[None], vgrad[None], ggrad


def solution(mesh):
    return jax.shard_map(
        local,
        mesh=mesh,
        in_specs=(
            P("section", "ctx", None),
            P("section", "ctx", None),
            P("section", "ctx", None),
            P("section", "ctx", None),
            P("section", "ctx"),
            P("section", "ctx"),
            P("section", "ctx"),
        ),
        out_specs=(P("section", "ctx", None), P("section", "ctx", None), P("section", "ctx")),
        check_vma=False,
    )
```

```python
import math

import jax
import jax.numpy as jnp
from jax import lax
from jax.experimental import pallas as pl
from jax.experimental.pallas import tpu as pltpu
from jax.sharding import PartitionSpec as P

GROUPS = 4
WIDE = 6
D = 128
B = 128
COLS = WIDE * D
SECTIONS = 8
CTX = 32
TILE = 2048
NB = TILE // B
LOW = -1e30
SCALE = math.log2(math.e) / math.sqrt(D)
BF = jnp.bfloat16
F32 = jnp.float32
NCOPY = 57
DIRECT = (0,)
Y_LARGE = (0, 1, 2, 3)


def kernel(
    counts, q_in, k_in, v_in, ct_in, lg_in,
    hz, hr, dvf, dvr, gs, fl, flr,
    cb, qs, qr, cs, cr, ks, kr, vs, vr, ls, lr, gr,
    kb, vb, sbuf, wbuf, qt, ot, dos, att_acc,
    pda, pdb, rba, rbb, ra, rb, ua, ub, ra2, rb2,
    br, csem, send_sems, recv_sems,
):
    sec = lax.axis_index("section")
    c = lax.axis_index("ctx")
    core = lax.rem(c, 2)
    y = lax.rem(lax.div(c, 2), 4)
    x = lax.div(c, 8)

    def dev(xx, yy, kk):
        return (sec, (lax.rem(xx + 8, 4) * 4 + lax.rem(yy + 8, 4)) * 2 + kk)

    nxt = (sec, lax.rem(c + 1, CTX))
    prv = (sec, lax.rem(c + CTX - 1, CTX))
    zup = (lax.rem(sec + 1, SECTIONS), c)
    zdn = (lax.rem(sec + SECTIONS - 1, SECTIONS), c)
    sib = (sec, c + 1 - 2 * core)
    MESH = pl.DeviceIdType.MESH

    sets = {
        "s1": kb.at[0, 0, pl.ds(0, 2), pl.ds(0, 3)],
        "s2": kb.at[0, 0, pl.ds(0, 2)],
        "s3": kb.at[0, 0, pl.ds(0, 2)],
        "s4": kb.at[0],
        "a0": pda.at[0],
        "a1": pda.at[0, pl.ds(0, 2), pl.ds(0, 3)],
        "a3": pda.at[0, 0, pl.ds(0, 2), pl.ds(0, 3)],
    }
    slots = {}

    def copy(name, src, dst, to):
        n, _ = slots.setdefault(name, (len(slots), sets.get(name[0], dst)))
        pltpu.make_async_remote_copy(
            src_ref=src, dst_ref=dst, send_sem=send_sems.at[n], recv_sem=recv_sems.at[n],
            device_id=to, device_id_type=MESH,
        ).start()

    def whole(name):
        n, ref = slots[name]
        return pltpu.make_async_remote_copy(
            src_ref=ref, dst_ref=ref, send_sem=send_sems.at[n], recv_sem=recv_sems.at[n],
            device_id=sib, device_id_type=MESH,
        )

    def arrived(*name):
        whole(name).wait_recv()

    bar = pltpu.get_barrier_semaphore()

    @pl.loop(1, CTX)
    def _(d):
        pl.semaphore_signal(bar, inc=1, device_id=(sec, lax.rem(c + d, CTX)), device_id_type=MESH)

    pl.semaphore_signal(bar, inc=1, device_id=zup, device_id_type=MESH)
    pl.semaphore_signal(bar, inc=1, device_id=zdn, device_id_type=MESH)

    held = counts[0, 0]
    two = held == 2
    cb[pl.ds(c, 1)] = jnp.full((1, 1, 128), held, jnp.int32)

    def pick(flag, a, b):
        return lax.select(jnp.broadcast_to(flag, a.shape), a, b)

    for g in range(GROUPS):
        kc = slice(g * D, (g + 1) * D)
        qc = slice(g * COLS, (g + 1) * COLS)
        ks[g] = pick(two, k_in[B:, kc], k_in[:B, kc])
        vs[g] = pick(two, v_in[B:, kc], v_in[:B, kc])
        qs[g] = pick(two, q_in[B:, qc], q_in[:B, qc])
        cs[g] = pick(two, ct_in[B:, qc], ct_in[:B, qc])
    lg = lg_in[...].astype(F32)
    ls[...] = jnp.broadcast_to(pick(two, lg[:, B:], lg[:, :B]), (8, 128))

    pl.semaphore_wait(bar, CTX + 1)

    @pl.loop(1, CTX)
    def _(d):
        pltpu.make_async_remote_copy(
            src_ref=cb.at[c], dst_ref=cb.at[c], send_sem=csem.at[0], recv_sem=csem.at[1],
            device_id=(sec, lax.rem(c + d, CTX)), device_id_type=MESH,
        ).start()

    copy(("k",), ks, kr, nxt)
    copy(("v",), vs, vr, nxt)
    copy(("l",), ls, lr, nxt)
    copy(("q", 0), qs.at[0], qr.at[0], nxt)

    every = pltpu.make_async_remote_copy(
        src_ref=cb.at[pl.ds(0, CTX - 1)], dst_ref=cb.at[pl.ds(0, CTX - 1)],
        send_sem=csem.at[0], recv_sem=csem.at[1], device_id=sib, device_id_type=MESH,
    )
    every.wait_recv()
    order = lax.broadcasted_iota(jnp.int32, (CTX, 1, 128), 0)
    ahead = jnp.sum(jnp.where(order < c, cb[...] - 1, 0), axis=0).astype(F32)
    before = jnp.max(ahead)
    late = before > 0.5
    held_f = held.astype(F32)
    fl[0] = jnp.broadcast_to(ahead, (8, 128))
    fl[1] = jnp.full((8, 128), held_f, F32)

    arrived("k")
    arrived("v")

    def at(v):
        return lax.rem(v + 8, 4)

    parts = {
        (kind, g): (kb if kind == "k" else vb, kind == "k" and g in Y_LARGE)
        for kind in ("k", "v")
        for g in range(GROUPS)
    }

    def place(kind, g):
        buf, y_large = parts[kind, g]
        small = (lambda d: dev(x + d, y, core)) if y_large else (lambda d: dev(x, y + d, core))
        large = (lambda d: dev(x, y + d, core)) if y_large else (lambda d: dev(x + d, y, core))
        return buf, y_large, (y, x) if y_large else (x, y), small, large

    def block(kind, g, kk, xx, yy):
        buf, y_large = parts[kind, g]
        return buf[g, kk, yy, xx] if y_large else buf[g, kk, xx, yy]

    for g in range(GROUPS):
        kc = slice(g * D, (g + 1) * D)
        for kind, got, own in (("k", kr, k_in), ("v", vr, v_in)):
            buf, _, (a, b), _, _ = place(kind, g)
            buf[g, core, a, b] = pick(late, got[g], own[:B, kc])
    copy(("f",), fl, flr, zup)

    def pass_q(g):
        pass_on("q", g)

    def pass_c(g):
        pass_on("c", g)

    def gather_one(g):
        for kind in ("k", "v"):
            buf, _, (a, b), small, _ = place(kind, g)
            own = buf.at[g, core, a, b]
            for d in (1, 3, 2):
                copy(("s1", g), own, own, small(d))

    def gather_second(g):
        arrived("s1", g)
        for d in (1, 3, 2) if g in DIRECT else (1, 3):
            for kind in ("k", "v"):
                buf, _, (a, b), _, large = place(kind, g)
                own = buf.at[g, core, a]
                copy(("s2", g, d), own, own, large(d))
        for kind in ("k", "v"):
            buf, _, (a, b), _, _ = place(kind, g)
            copy(("s4", g), buf.at[g, core, a], buf.at[g, core, a], sib)

    def gather_third(g):
        for d in (1, 3):
            arrived("s2", g, d)
            for kind in ("k", "v"):
                buf, _, (a, b), _, large = place(kind, g)
                aa = at(a - d)
                came = buf.at[g, core, aa]
                if g not in DIRECT:
                    half = buf.at[g, core, aa, pl.ds(d - 1, 2)]
                    copy(("s3", g), half, half, large(d))
                copy(("s4", g), came, came, sib)

    def gather_fourth(g):
        if g in DIRECT:
            arrived("s2", g, 2)
        else:
            arrived("s3", g)
        for kind in ("k", "v"):
            buf, _, (a, b), _, _ = place(kind, g)
            aa = at(a + 2)
            copy(("s4", g), buf.at[g, core, aa], buf.at[g, core, aa], sib)

    def gather_last(g):
        arrived("s4", g)

    def pass_on(name, g):
        if name == "q":
            copy(("q", g), qs.at[g], qr.at[g], nxt)
        else:
            copy(("c", g), cs.at[g], cr.at[g], nxt)

    tiles = lax.div(c, NB) + 1
    lane = lax.broadcasted_iota(jnp.int32, (TILE, 2 * D), 1)
    gap = lax.broadcasted_iota(jnp.int32, (TILE, 2 * D), 0) - lax.rem(lane, D)

    def forward(g, between, after):
        arrived("q", g)
        qc = slice(g * COLS, (g + 1) * COLS)
        for h in range(WIDE):
            hc = slice(h * D, (h + 1) * D)
            full = pick(late, qr[g, :, hc], q_in[:B, g * COLS + h * D : g * COLS + (h + 1) * D])
            full = (full.astype(F32) * SCALE).T
            high = full.astype(BF)
            qt[:D, hc] = high
            qt[D:, hc] = (full - high.astype(F32)).astype(BF)

        def scores(j, tops):
            xx = j * 2
            one = jnp.concatenate(
                [block("k", g, n % 2, xx + n // 8, n % 8 // 2) for n in range(NB)], axis=0
            )
            both = jnp.concatenate([one, one], axis=1)
            bound = c * B - j * TILE
            out = []
            for p in range(3):
                pc = slice(p * 2 * D, (p + 1) * 2 * D)
                s = jnp.dot(both, qt[:, pc], preferred_element_type=F32)
                s = jnp.where(gap <= bound, s, LOW)
                sbuf[pl.ds(pl.multiple_of(j * TILE, TILE), TILE), pc] = s
                out.append(jnp.maximum(tops[p], jnp.max(s.reshape(TILE // 8, 8, 2 * D), axis=0)))
            return tuple(out)

        tops = lax.fori_loop(
            0, tiles, scores, tuple(jnp.full((8, 2 * D), LOW, F32) for _ in range(3))
        )
        tops = [jnp.max(t, axis=0, keepdims=True) for t in tops]
        ot[...] = jnp.zeros_like(ot)
        between()

        def weigh(j, _):
            xx = j * 2
            one = jnp.concatenate(
                [block("v", g, n % 2, xx + n // 8, n % 8 // 2) for n in range(NB)], axis=0
            )
            left = jnp.concatenate([one.T, jnp.ones((16, TILE), BF)], axis=0)
            rows = pl.ds(pl.multiple_of(j * TILE, TILE), TILE)
            for p in range(3):
                pc = slice(p * 2 * D, (p + 1) * 2 * D)
                w = jnp.exp2(sbuf[rows, pc] - tops[p]).astype(BF)
                wbuf[rows, pc] = w
                ot[:, pc] += jnp.dot(left, w, preferred_element_type=F32)
            return 0

        lax.fori_loop(0, tiles, weigh, 0)
        after()
        if g == 0:
            arrived("l")
            gate_row = 1.0 / (1.0 + jnp.exp(-pick(late, lr[...], jnp.broadcast_to(lg[:, :B], (8, 128)))))
            gr[...] = gate_row
            att_acc[0] = jnp.broadcast_to(gate_row[:1], (B, D)).T
            att_acc[1] = jnp.zeros((B, D), F32)
        arrived("c", g)
        gate = att_acc[0]
        acc = att_acc[1]
        for h in range(WIDE):
            hc = slice(h * D, (h + 1) * D)
            inv = 1.0 / ot[D : D + 1, hc]
            attended = (ot[:D, hc] * inv).T
            br[g, :, hc] = (gate * attended).astype(BF)
            ct = pick(late, cr[g, :, hc], ct_in[:B, g * COLS + h * D : g * COLS + (h + 1) * D]).astype(F32)
            acc = acc + ct * attended
            dos[hc, :] = (gate * ct * jnp.broadcast_to(inv, (B, D)).T).astype(BF)
        att_acc[1] = acc
        copy(("h", g), br.at[g], hz.at[:, g * COLS : (g + 1) * COLS], zup)

    def backward(g):
        def terms(j, _):
            xx = j * 2
            rows = pl.ds(pl.multiple_of(j * TILE, TILE), TILE)
            t = jnp.dot(wbuf[rows, :], dos[...], preferred_element_type=F32).astype(BF)
            for n in range(NB):
                pda[g, n % 2, xx + n // 8, n % 8 // 2] = t[n * B : n * B + 64]
                pdb[g, n % 2, n % 8 // 2, xx + n // 8] = t[n * B + 64 : (n + 1) * B]
            return 0

        lax.fori_loop(0, tiles, terms, 0)

        def blank(j, _):
            xx = j * 2
            for n in range(NB):
                pda[g, n % 2, xx + n // 8, n % 8 // 2] = jnp.zeros((64, D), BF)
                pdb[g, n % 2, n % 8 // 2, xx + n // 8] = jnp.zeros((64, D), BF)
            return 0

        lax.fori_loop(tiles, CTX // NB, blank, 0)
        copy(("a0", g), pda.at[g, 1 - core], rba.at[g], sib)
        copy(("a0", g), pdb.at[g, 1 - core], rbb.at[g], sib)

    def reduce_first(g):
        arrived("a0", g)
        rba[g] = (pda[g, core].astype(F32) + rba[g].astype(F32)).astype(BF)
        rbb[g] = (pdb[g, core].astype(F32) + rbb[g].astype(F32)).astype(BF)
        for d in (2, 1, 3):
            copy(("a1", g), rba.at[g, at(x + d)], ra.at[g, d - 1], dev(x + d, y, core))
            copy(("a1", g), rbb.at[g, at(y + d)], rb.at[g, d - 1], dev(x, y + d, core))

    def reduce_second(g):
        suma = rba[g, x].astype(F32)
        sumb = rbb[g, y].astype(F32)
        arrived("a1", g)
        for d in (1, 3, 2):
            suma = suma + ra[g, d - 1].astype(F32)
            sumb = sumb + rb[g, d - 1].astype(F32)
        ua[g] = suma.astype(BF)
        ub[g] = sumb.astype(BF)
        for d in (2, 1, 3):
            copy(("a3", g), ua.at[g, at(y + d)], ra2.at[g, d - 1], dev(x, y + d, core))
            copy(("a3", g), ub.at[g, at(x + d)], rb2.at[g, d - 1], dev(x + d, y, core))

    def reduce_third(g):
        suma = ua[g, y].astype(F32)
        sumb = ub[g, x].astype(F32)
        arrived("a3", g)
        for d in (1, 3, 2):
            suma = suma + ra2[g, d - 1].astype(F32)
            sumb = sumb + rb2[g, d - 1].astype(F32)
        kc = slice(g * D, (g + 1) * D)
        dvf[:64, kc] = suma.astype(BF)
        dvf[64:, kc] = sumb.astype(BF)
        copy(("r", g), dvf.at[:, kc], dvr.at[:, kc], prv)

    def hand_on(g):
        oc = slice(g * COLS, (g + 1) * COLS)
        arrived("h", g)
        copy(("h2", g), hz.at[:, oc], hr.at[:, oc], prv)

    def gate_out():
        gate_row = gr[...]
        total = jnp.sum(att_acc[1].T, axis=0, keepdims=True)
        ls_row = gate_row * (1.0 - gate_row) * jnp.broadcast_to(total, (8, 128))
        gs[0] = ls_row
        copy(("g",), gs.at[0], gs.at[1], prv)

    gather_one(0)
    gather_second(0)
    gather_one(1)
    gather_third(0)
    gather_one(2)
    gather_second(1)
    pass_on("c", 0)
    gather_fourth(0)
    gather_one(3)
    gather_last(0)
    plan = {
        (0, 0): [(gather_third, 1), (gather_second, 2), (pass_q, 1)],
        (0, 1): [(pass_c, 1)],
        (0, 2): [(gather_fourth, 1), (gather_second, 3)],
        (0, 3): [(gather_third, 2), (gather_last, 1), (pass_q, 2), (pass_c, 2)],
        (1, 0): [(reduce_first, 0)],
        (1, 1): [(gather_third, 3), (hand_on, 0)],
        (1, 2): [(gather_fourth, 2), (pass_q, 3), (pass_c, 3)],
        (1, 3): [(reduce_second, 0), (gather_last, 2)],
        (2, 0): [(reduce_first, 1), (gather_fourth, 3)],
        (2, 1): [(reduce_third, 0), (hand_on, 1)],
        (2, 2): [(gather_last, 3)],
        (2, 3): [(reduce_second, 1)],
        (3, 0): [(reduce_first, 2)],
        (3, 1): [(reduce_third, 1), (hand_on, 2)],
        (3, 2): [(reduce_second, 2)],
        (3, 3): [],
    }
    for g in range(GROUPS):
        def at_slot(n):
            for what, k in plan[g, n]:
                what(k)

        forward(g, lambda: at_slot(0), lambda: at_slot(1))
        at_slot(2)
        backward(g)
        if g == GROUPS - 1:
            gate_out()
        at_slot(3)
    last = GROUPS - 1
    reduce_first(last)
    reduce_third(2)
    reduce_second(last)
    hand_on(last)
    reduce_third(last)
    arrived("f")
    arrived("g")
    for g in range(GROUPS):
        arrived("h2", g)
        arrived("r", g)

    every.wait_send()
    for name in slots:
        whole(name).wait_send()


def finish(hz, hr, dvf, dvr, gs, fl, flr, handed, vgrad, ggrad):
    def slotted(flags, mine, back, out, cols):
        first, held = jnp.max(flags[0]), jnp.max(flags[1])
        carried = first + held > 1.5
        one = jnp.logical_and(carried, jnp.logical_and(held > 0.5, held < 1.5))
        both = jnp.logical_and(carried, held > 1.5)
        nothing = jnp.zeros_like(mine)

        def pick(flag, a, b):
            return lax.select(jnp.broadcast_to(flag, a.shape), a, b)

        out(pick(first < 0.5, mine, pick(one, back, nothing)), pick(both, back, nothing), cols)

    def rows(ref):
        def put(top, low, cols):
            ref[:B, cols] = top
            ref[B:, cols] = low

        return put

    def lanes(top, low, cols):
        ggrad[:, :B] = top.astype(BF)
        ggrad[:, B:] = low.astype(BF)

    for n in range(GROUPS * WIDE):
        cols = slice(n * D, (n + 1) * D)
        slotted(flr, hz[:, cols], hr[:, cols], rows(handed), cols)
    for n in range(GROUPS):
        cols = slice(n * D, (n + 1) * D)
        slotted(fl, dvf[:, cols], dvr[:, cols], rows(vgrad), cols)
    slotted(fl, gs[0, :1], gs[1, :1], lanes, None)


def local(queries, keys, values, cotangent, router_logits, positions, counts):
    del positions
    V = pl.BlockSpec(memory_space=pltpu.VMEM)
    G = GROUPS
    vm = pltpu.VMEM
    scratch = [
        vm((CTX, 1, 128), jnp.int32),
        vm((G, B, COLS), BF), vm((G, B, COLS), BF), vm((G, B, COLS), BF), vm((G, B, COLS), BF),
        vm((G, B, D), BF), vm((G, B, D), BF), vm((G, B, D), BF), vm((G, B, D), BF),
        vm((8, 128), F32), vm((8, 128), F32), vm((8, 128), F32),
        vm((G, 2, 4, 4, B, D), BF), vm((G, 2, 4, 4, B, D), BF),
        vm((CTX * B, COLS), F32), vm((CTX * B, COLS), BF),
        vm((2 * D, COLS), BF), vm((D + 16, COLS), F32), vm((COLS, D), BF), vm((2, B, D), F32),
        vm((G, 2, 4, 4, 64, D), BF), vm((G, 2, 4, 4, 64, D), BF),
        vm((G, 4, 4, 64, D), BF), vm((G, 4, 4, 64, D), BF),
        vm((G, 3, 4, 64, D), BF), vm((G, 3, 4, 64, D), BF),
        vm((G, 4, 64, D), BF), vm((G, 4, 64, D), BF),
        vm((G, 3, 64, D), BF), vm((G, 3, 64, D), BF),
        vm((G, B, COLS), BF),
        pltpu.SemaphoreType.DMA((2,)),
        pltpu.SemaphoreType.DMA((NCOPY,)),
        pltpu.SemaphoreType.DMA((NCOPY,)),
    ]
    hz, hr, dvf, dvr, gs, fl, flr = pl.pallas_call(
        kernel,
        out_shape=(
            jax.ShapeDtypeStruct((B, G * COLS), BF),
            jax.ShapeDtypeStruct((B, G * COLS), BF),
            jax.ShapeDtypeStruct((B, G * D), BF),
            jax.ShapeDtypeStruct((B, G * D), BF),
            jax.ShapeDtypeStruct((2, 8, 128), F32),
            jax.ShapeDtypeStruct((2, 8, 128), F32),
            jax.ShapeDtypeStruct((2, 8, 128), F32),
        ),
        in_specs=[pl.BlockSpec(memory_space=pltpu.SMEM)] + [V] * 5,
        out_specs=(V,) * 7,
        scratch_shapes=scratch,
        compiler_params=pltpu.CompilerParams(
            collective_id=0, has_side_effects=True, vmem_limit_bytes=66_000_000
        ),
        name="routed_block",
    )(counts, queries[0], keys[0], values[0], cotangent[0], router_logits)
    handed, vgrad, ggrad = pl.pallas_call(
        finish,
        out_shape=(
            jax.ShapeDtypeStruct((2 * B, G * COLS), BF),
            jax.ShapeDtypeStruct((2 * B, G * D), BF),
            jax.ShapeDtypeStruct((1, 2 * B), BF),
        ),
        in_specs=[V] * 7,
        out_specs=(V, V, V),
        name="slots",
    )(hz, hr, dvf, dvr, gs, fl, flr)
    return handed[None], vgrad[None], ggrad


def solution(mesh):
    return jax.shard_map(
        local,
        mesh=mesh,
        in_specs=(
            P("section", "ctx", None),
            P("section", "ctx", None),
            P("section", "ctx", None),
            P("section", "ctx", None),
            P("section", "ctx"),
            P("section", "ctx"),
            P("section", "ctx"),
        ),
        out_specs=(P("section", "ctx", None), P("section", "ctx", None), P("section", "ctx")),
        check_vma=False,
    )
```
